256 devices in a mesh: ch: 128 (over x, y_lo, z, core), rep: 2 (over y_hi).
Axes of the slice: x: 4, y: 4 (y_hi: 2, y_lo: 2; y = y_hi * 2 + y_lo), z: 8, core: 2. Of those that a mesh axis runs over, the one named last changes fastest.
Arguments:
- fields_a: bfloat16 [32, 128, 32768], P('rep', 'ch'), parts along dimension 0, may hold values from -6 to 6
- latent_b: bfloat16 [32, 16384, 512], P('rep', 'ch'), parts along dimension 0, may hold values from -6 to 6
- regrid_w: bfloat16 [256, 1, 128, 64], replicated, may hold values from -0.5 to 0.5
- cell_tiles: int32 [256, 1], replicated, may hold values from 0 to 255, as said below
- norm_a: float32 [128], replicated, may hold values from 0.5 to 1.5
- enc_in: bfloat16 [128, 512], replicated, may hold values from -0.5 to 0.5
- enc_mid: bfloat16 [512, 512], replicated, may hold values from -0.25 to 0.25
- enc_out: bfloat16 [512, 512], replicated, may hold values from -0.25 to 0.25
- norm_b: float32 [512], replicated, may hold values from 0.5 to 1.5
- dec_mid: bfloat16 [512, 512], replicated, may hold values from -0.25 to 0.25
- dec_out: bfloat16 [512, 128], replicated, may hold values from -0.25 to 0.25
Outputs:
- latent_a: bfloat16 [32, 16384, 512], P('rep', 'ch'), parts along dimension 0
- cells_b: bfloat16 [32, 128, 32768], P('rep', 'ch'), parts along dimension 0
The draws below stay inside these ranges and needn't reach their ends.
There are 2 independent parts, one for each index of `rep`. The reference program is written for one: setup_inputs(seed, part) draws one part's arguments, and reference() takes and returns one part's arrays. A program takes and returns all parts, laid end to end along the dimension named above; an argument that names none is the same for every part. Nothing has to cross between parts.
Inputs may be any that keep to these rules, and one draw needn't show every extreme that they name: The one column of cell_tiles names every one of the 256 cell blocks exactly once.
All inputs are finite; a program needn't handle non-finite values.
Results may differ from the reference program's by a relative error of at most 0.0066.
Values may be sent and summed in bfloat16 or wider, within the bound.
A program may use at most 64 MiB of HBM per device.

```python
import jax
import jax.numpy as jnp
from jax import lax

CHANNELS = 128
HIDDEN_SIZE = 512
ENS = 16
BN = 64
BC = 128
K = 1
NODES = 16384
NB = 256
CELLS = 32768


def draw_cell_tiles(key, part):
    columns = [jax.random.permutation(jax.random.fold_in(key, 11 + column), NB) for column in range(K)]
    return jnp.stack(columns, axis=1).astype(jnp.int32)


def block_scale(key, extent, cuts, least, largest):
    loudness, own = 1.0, jax.random.fold_in(key, 6)
    for position, blocks in cuts:
        heights = jnp.exp(jax.random.uniform(jax.random.fold_in(own, position), (blocks,), jnp.float32, least / len(cuts), largest / len(cuts)))
        loudness = loudness * jnp.repeat(heights, extent[position] // blocks).reshape([-1 if axis == position else 1 for axis in range(len(extent))])
    return loudness


def normal_values(key, dims, scale, limit, cuts=(), kind=jnp.bfloat16):
    result = scale * jax.random.normal(key, dims, jnp.float32)
    if cuts:
        result = result * block_scale(key, dims, cuts, -0.22, 0.18)
    return jnp.clip(result, -limit, limit).astype(kind)


def setup_inputs(seed: int = 0, part: int = 0) -> dict:
    seeds = jax.random.split(jax.random.key(seed), 12)
    own_keys = jax.random.split(jax.random.fold_in(seeds[11], part), 12)
    return {
        "fields_a": normal_values(own_keys[0], (ENS, CHANNELS, CELLS), 1.0, 6.0, ((1, 128),)),
        "latent_b": normal_values(own_keys[1], (ENS, NODES, HIDDEN_SIZE), 1.0, 6.0, ((1, 128),)),
        "regrid_w": normal_values(seeds[2], (NB, K, BC, BN), (K * BC) ** -0.5, 0.5),
        "cell_tiles": draw_cell_tiles(jax.random.fold_in(seeds[11], 71), part),
        "norm_a": jnp.clip(1.0 + 0.1 * jax.random.normal(seeds[4], (CHANNELS,), jnp.float32), 0.5, 1.5),
        "enc_in": normal_values(seeds[5], (CHANNELS, HIDDEN_SIZE), CHANNELS ** -0.5, 0.5),
        "enc_mid": normal_values(seeds[6], (HIDDEN_SIZE, HIDDEN_SIZE), HIDDEN_SIZE ** -0.5, 0.25),
        "enc_out": normal_values(seeds[7], (HIDDEN_SIZE, HIDDEN_SIZE), HIDDEN_SIZE ** -0.5, 0.25),
        "norm_b": jnp.clip(1.0 + 0.1 * jax.random.normal(seeds[8], (HIDDEN_SIZE,), jnp.float32), 0.5, 1.5),
        "dec_mid": normal_values(seeds[9], (HIDDEN_SIZE, HIDDEN_SIZE), HIDDEN_SIZE ** -0.5, 0.25),
        "dec_out": normal_values(seeds[10], (HIDDEN_SIZE, CHANNELS), HIDDEN_SIZE ** -0.5, 0.25),
    }


EPSILON = 1e-05

def normalize(values, gain_vec, along):
    average = lax.optimization_barrier(jnp.mean(values, axis=along, keepdims=True))
    centred = values - average
    spread = lax.optimization_barrier(jnp.mean(centred * centred, axis=along, keepdims=True))
    return centred * lax.rsqrt(spread + EPSILON) * gain_vec

def reference(fields_a, latent_b, regrid_w, cell_tiles, norm_a, enc_in, enc_mid, enc_out, norm_b, dec_mid, dec_out):
    blocks = fields_a.reshape(ENS, CHANNELS, NB, BC)
    chosen = jnp.take(blocks, cell_tiles, axis=2).reshape(ENS, CHANNELS, NB, K * BC)
    weights = regrid_w.reshape(NB, K * BC, BN)
    grid_a = jnp.einsum('ecnj,njm->ecnm', chosen.astype(jnp.float32), weights.astype(jnp.float32), precision=lax.Precision.HIGHEST).astype(jnp.bfloat16)
    grid_a = grid_a.reshape(ENS, CHANNELS, NODES)

    def encode_one(grid_one):
        values = grid_one.T.astype(jnp.float32)
        normed = normalize(values, norm_a, -1).astype(jnp.bfloat16)
        base = jnp.dot(normed, enc_in, preferred_element_type=jnp.float32).astype(jnp.bfloat16)
        middle = jax.nn.silu(jnp.dot(base, enc_mid, preferred_element_type=jnp.float32)).astype(jnp.bfloat16)
        return (base.astype(jnp.float32) + jnp.dot(middle, enc_out, preferred_element_type=jnp.float32)).astype(jnp.bfloat16)
    latent_a = lax.map(encode_one, grid_a)

    def decode_one(latent_one):
        normed = normalize(latent_one.astype(jnp.float32), norm_b, -1).astype(jnp.bfloat16)
        middle = jax.nn.silu(jnp.dot(normed, dec_mid, preferred_element_type=jnp.float32)).astype(jnp.bfloat16)
        return jnp.dot(middle, dec_out, preferred_element_type=jnp.float32).astype(jnp.bfloat16)
    nodes_b = lax.map(decode_one, latent_b)
    node_blocks = jnp.transpose(nodes_b, (0, 2, 1)).reshape(ENS, CHANNELS, NB, BN)
    inverse = jnp.argsort(cell_tiles, axis=0).astype(jnp.int32).T
    picked = jnp.take(node_blocks, inverse, axis=2)
    weight_sel = regrid_w[inverse, jnp.arange(K).astype(jnp.int32)[:, None]]
    total = jnp.einsum('ecknm,knbm->ecnb', picked.astype(jnp.float32), weight_sel.astype(jnp.float32), precision=lax.Precision.HIGHEST)
    cells_b = total.astype(jnp.bfloat16).reshape(ENS, CHANNELS, CELLS)
    return (latent_a, cells_b)
```

```python
import functools

import jax
import jax.numpy as jnp
from jax import lax
from jax.experimental import pallas as pl
from jax.experimental.pallas import tpu as pltpu
from jax.sharding import PartitionSpec as P

BN = 64
BC = 128
K = 1


EPSILON = 1e-05


def normalize(values, gain_vec, along):
    average = jnp.mean(values, axis=along, keepdims=True)
    centred = values - average
    spread = jnp.mean(centred * centred, axis=along, keepdims=True)
    return centred * lax.rsqrt(spread + EPSILON) * gain_vec


def exchange_body(groups, a_ref, b_ref, got_a, got_b, send_sem, recv_a, recv_b):
    me = lax.axis_index("ch")
    barrier = pltpu.get_barrier_semaphore()

    def greet(step, carry):
        peer = {"ch": lax.rem(me + step, groups)}
        pl.semaphore_signal(barrier, inc=1, device_id=peer, device_id_type=pl.DeviceIdType.MESH)
        return carry

    lax.fori_loop(1, groups, greet, 0)
    got_a[me] = a_ref[me]
    got_b[me] = b_ref[me]
    pl.semaphore_wait(barrier, groups - 1)
    for sent, got, sem in ((a_ref, got_a, recv_a), (b_ref, got_b, recv_b)):

        def send(step, carry):
            peer = lax.rem(me + step, groups)
            pltpu.make_async_remote_copy(
                src_ref=sent.at[peer],
                dst_ref=got.at[me],
                send_sem=send_sem,
                recv_sem=sem,
                device_id={"ch": peer},
                device_id_type=pl.DeviceIdType.MESH,
            ).start()
            return carry

        lax.fori_loop(1, groups, send, 0)
    for sent, got, sem in ((a_ref, got_a, recv_a), (b_ref, got_b, recv_b)):
        most = pl.ds(0, groups - 1)
        pltpu.make_async_copy(sent.at[most], got.at[most], sem).wait()
        pltpu.make_async_copy(sent.at[most], got.at[most], send_sem).wait()


def exchange(a, b):
    groups = a.shape[0]
    whole = pl.BlockSpec(memory_space=pltpu.VMEM)
    return pl.pallas_call(
        functools.partial(exchange_body, groups),
        out_shape=[jax.ShapeDtypeStruct(a.shape, a.dtype)] * 2,
        in_specs=[whole] * 2,
        out_specs=[whole] * 2,
        scratch_shapes=[pltpu.SemaphoreType.DMA] * 3,
        compiler_params=pltpu.CompilerParams(collective_id=0, has_side_effects=True),
        name="exchange",
    )(a, b)


def shards(
    fields_a,
    latent_b,
    regrid_w,
    cell_tiles,
    norm_a,
    enc_in,
    enc_mid,
    enc_out,
    norm_b,
    dec_mid,
    dec_out,
):
    groups = lax.axis_size("ch")
    samples = fields_a.shape[0]
    own_channels = fields_a.shape[1]
    blocks_all = cell_tiles.shape[0]
    node_rows = latent_b.shape[1]
    hidden = latent_b.shape[2]
    channels = own_channels * groups
    blocks = fields_a.reshape(samples, own_channels, blocks_all, BC)
    chosen = jnp.take(blocks, cell_tiles, axis=2).reshape(samples, own_channels, blocks_all, K * BC)
    weights = regrid_w.reshape(blocks_all, K * BC, BN)
    grid_vals = jnp.einsum("ecnj,njm->ecnm", chosen, weights, preferred_element_type=jnp.float32)
    grid_sent = grid_vals.astype(jnp.bfloat16).reshape(samples, own_channels, groups, node_rows)
    normed = normalize(latent_b.astype(jnp.float32), norm_b, 2).astype(jnp.bfloat16)
    middle = jax.nn.silu(
        jnp.einsum("enh,hg->eng", normed, dec_mid, preferred_element_type=jnp.float32)
    ).astype(jnp.bfloat16)
    out_split = dec_out.reshape(hidden, groups, own_channels)
    decoded_sent = jnp.einsum(
        "enh,hjc->ecjn", middle, out_split, preferred_element_type=jnp.float32
    ).astype(jnp.bfloat16)
    received_a, received_b = exchange(
        jnp.transpose(grid_sent.reshape(samples, groups, node_rows), (1, 0, 2)),
        jnp.transpose(decoded_sent.reshape(samples, groups, node_rows), (1, 0, 2)),
    )
    values = received_a.astype(jnp.float32)
    normed = normalize(values, norm_a[:, None, None], 0).astype(jnp.bfloat16)
    base = jnp.einsum("cen,ch->enh", normed, enc_in, preferred_element_type=jnp.float32).astype(
        jnp.bfloat16
    )
    middle = jax.nn.silu(
        jnp.einsum("enh,hg->eng", base, enc_mid, preferred_element_type=jnp.float32)
    ).astype(jnp.bfloat16)
    result = base.astype(jnp.float32) + jnp.einsum(
        "enh,hg->eng", middle, enc_out, preferred_element_type=jnp.float32
    )
    latent_a = result.astype(jnp.bfloat16)
    node_blocks = jnp.moveaxis(received_b, 0, 1).reshape(samples, own_channels, blocks_all, BN)
    inverse = jnp.argsort(cell_tiles, axis=0).T
    picked = jnp.take(node_blocks, inverse, axis=2)
    weight_sel = regrid_w[inverse, jnp.arange(K)[:, None]]
    total = jnp.einsum("ecknm,knbm->ecnb", picked, weight_sel, preferred_element_type=jnp.float32)
    cells_b = total.astype(jnp.bfloat16).reshape(samples, own_channels, blocks_all * BC)
    return (latent_a, cells_b)


def solution(mesh):
    placed = (
        P("rep", "ch", None),
        P("rep", "ch", None),
        P(),
        P(),
        P(),
        P(),
        P(),
        P(),
        P(),
        P(),
        P(),
    )
    return jax.shard_map(
        shards,
        mesh=mesh,
        in_specs=placed,
        out_specs=(P("rep", "ch", None), P("rep", "ch", None)),
        check_vma=False,
    )
```

```python
import functools

import jax
import jax.numpy as jnp
from jax import lax
from jax.experimental import pallas as pl
from jax.experimental.pallas import tpu as pltpu
from jax.sharding import PartitionSpec as P

BN = 64
BC = 128
EPSILON = 1e-05
BATCH = 8
CHUNK = 16
PITCH_A = 24
PITCH_B = 136
NT = (((1,), (1,)), ((), ()))
MESH = pl.DeviceIdType.MESH


in_hbm = functools.partial(pltpu.with_memory_space_constraint, memory_space=pltpu.HBM)
in_vmem = functools.partial(pltpu.with_memory_space_constraint, memory_space=pltpu.VMEM)


def silu(v):
    return v / (1.0 + jnp.exp(-v))


def main_body(
    groups,
    tiles_h,
    fields_h,
    regrid_h,
    latent_h,
    norm_a_h,
    enc_in_h,
    enc_mid_h,
    enc_out_h,
    norm_b_h,
    dec_mid_h,
    dec_out_h,
    latent_o,
    cells_o,
    tiles,
    norm_a,
    fields,
    regrid,
    latent,
    enc_in,
    enc_mid,
    enc_out,
    norm_b,
    dec_mid,
    dec_out,
    sent_a,
    sent_b,
    got_a,
    got_b,
    stage_a,
    stage_b,
    load_sem,
    regrid_sem,
    send_sem,
    recv_a,
    recv_b,
):
    me = lax.axis_index("ch")
    samples, nodes = latent.shape[:2]
    chunks = groups // CHUNK
    batches = groups // BATCH

    def load(k, src, dst):
        copy = pltpu.make_async_copy(src, dst, load_sem.at[k])
        copy.start()
        return copy

    load_tiles = load(0, tiles_h, tiles)
    load_fields = load(1, fields_h, fields)
    load_regrid = []
    for k in range(chunks):
        part = pl.ds(lax.rem(me // CHUNK + k, chunks) * CHUNK, CHUNK)
        copy = pltpu.make_async_copy(regrid_h.at[part], regrid.at[part], regrid_sem.at[k])
        copy.start()
        load_regrid.append(copy)
    load_dec = [
        load(2, latent_h, latent),
        load(3, norm_b_h, norm_b),
        load(4, dec_mid_h, dec_mid),
        load(5, dec_out_h, dec_out),
    ]
    load_enc = [
        load(6, norm_a_h, norm_a),
        load(7, enc_in_h, enc_in),
        load(8, enc_mid_h, enc_mid),
        load(9, enc_out_h, enc_out),
    ]

    barrier = pltpu.get_barrier_semaphore()

    def greet(step, carry):
        peer = {"ch": lax.rem(me + step, groups)}
        pl.semaphore_signal(barrier, inc=1, device_id=peer, device_id_type=MESH)
        return carry

    lax.fori_loop(1, groups, greet, 0)

    left_half = lax.broadcasted_iota(jnp.int32, (samples, BC), 1) < BN

    def send(sent, got, sem_of):
        def one(step, carry):
            peer = lax.rem(me + step, groups)
            pltpu.make_async_remote_copy(
                src_ref=sent.at[peer],
                dst_ref=got.at[me],
                send_sem=send_sem,
                recv_sem=sem_of(step),
                device_id={"ch": peer},
                device_id_type=MESH,
            ).start()
            return carry

        return one

    send_a = send(sent_a, got_a, lambda step: recv_a)
    send_b = send(sent_b, got_b, lambda step: recv_b.at[step // BATCH])

    def regrid_batch(batch):
        for j in range(BATCH):
            d = lax.rem(me + batch * BATCH + j, groups)
            blocks = [tiles[2 * d], tiles[2 * d + 1]]
            x = [fields[rows, block] for block in blocks for rows in range(fields.shape[0])]
            both = lax.dot_general(
                jnp.concatenate(x, axis=0), regrid[d], NT, preferred_element_type=jnp.float32
            )
            mine = jnp.where(left_half, both[:samples], both[samples:])
            sent_a[d] = mine.astype(jnp.bfloat16)

    load_tiles.wait()
    load_fields.wait()
    load_regrid[0].wait()
    half_way = batches // 2
    per_chunk = CHUNK // BATCH
    for batch in range(half_way):
        if batch % per_chunk == 0:
            load_regrid[batch // per_chunk + 1].wait()
        regrid_batch(batch)
    got_a[me] = sent_a[me]
    pl.semaphore_wait(barrier, groups - 1)
    for batch in range(half_way, batches):
        if batch % per_chunk == 0 and batch // per_chunk + 1 < chunks:
            load_regrid[batch // per_chunk + 1].wait()
        regrid_batch(batch)
        done = 2 * (batch - half_way) * BATCH
        lax.fori_loop(max(1, done - BATCH), done + BATCH, send_a, 0)
    lax.fori_loop(groups - BATCH, groups, send_a, 0)

    for copy in load_dec:
        copy.wait()

    def decode(e, carry):
        v = latent[e].astype(jnp.float32)
        centred = v - jnp.mean(v, axis=1, keepdims=True)
        spread = jnp.mean(centred * centred, axis=1, keepdims=True)
        normed = (centred * lax.rsqrt(spread + EPSILON) * norm_b[...]).astype(jnp.bfloat16)
        middle = silu(jnp.dot(normed, dec_mid[...], preferred_element_type=jnp.float32))
        out = jnp.dot(
            middle.astype(jnp.bfloat16), dec_out[...], preferred_element_type=jnp.float32
        )
        stage_b[pl.ds(pl.multiple_of(e * PITCH_B, 8), groups), :] = out.T
        return carry

    lax.fori_loop(0, samples, decode, 0)

    def pack_batch(batch, carry):
        for j in range(BATCH):
            c = lax.rem(me + batch * BATCH + j, groups)
            rows = stage_b[pl.ds(c, samples, stride=PITCH_B), :]
            sent_b[c] = rows.astype(jnp.bfloat16)
        lax.fori_loop(
            jnp.maximum(1, (batch - 1) * BATCH), jnp.maximum(1, batch * BATCH), send_b, 0
        )
        return carry

    lax.fori_loop(0, batches, pack_batch, 0)
    lax.fori_loop(groups - BATCH, groups, send_b, 0)
    got_b[me] = sent_b[me]

    for copy in load_enc:
        copy.wait()
    most = pl.ds(0, groups - 1)
    pltpu.make_async_copy(sent_a.at[most], got_a.at[most], recv_a).wait()

    def add(c, total):
        return total + got_a[c].astype(jnp.float32)

    zero = jnp.zeros((samples, nodes), jnp.float32)
    average = lax.fori_loop(0, groups, add, zero, unroll=8) / groups

    def add_square(c, total):
        centred = got_a[c].astype(jnp.float32) - average
        return total + centred * centred

    spread = lax.fori_loop(0, groups, add_square, zero, unroll=8) / groups
    factor = lax.rsqrt(spread + EPSILON)

    def scale(c, carry):
        centred = got_a[c].astype(jnp.float32) - average
        rows = pl.ds(pl.multiple_of(c * PITCH_A, 8), samples)
        stage_a[rows, :] = centred * factor * norm_a[c]
        return carry

    lax.fori_loop(0, groups, scale, 0, unroll=8)

    def encode(e, carry):
        normed = stage_a[pl.ds(e, groups, stride=PITCH_A), :].T.astype(jnp.bfloat16)
        base = jnp.dot(normed, enc_in[...], preferred_element_type=jnp.float32).astype(jnp.bfloat16)
        middle = silu(jnp.dot(base, enc_mid[...], preferred_element_type=jnp.float32))
        out = base.astype(jnp.float32) + jnp.dot(
            middle.astype(jnp.bfloat16), enc_out[...], preferred_element_type=jnp.float32
        )
        latent_o[e] = out.astype(jnp.bfloat16)
        return carry

    lax.fori_loop(0, samples, encode, 0)

    def regrid_back(batch, carry):
        for j in range(BATCH):
            s = lax.rem(me + groups - batch * BATCH - j, groups)
            x = got_b[s]
            none = jnp.zeros_like(x)
            split = jnp.concatenate([jnp.where(left_half, x, none), jnp.where(left_half, none, x)], axis=0)
            cells = jnp.dot(split, regrid[s], preferred_element_type=jnp.float32)
            cells_o[s] = cells.astype(jnp.bfloat16)
        return carry

    def wait_back(batch, count):
        part = pl.ds(0, count)
        pltpu.make_async_copy(sent_b.at[part], got_b.at[part], recv_b.at[batch]).wait()

    wait_back(0, BATCH - 1)
    regrid_back(0, 0)

    def back(batch, carry):
        wait_back(batch, BATCH)
        return regrid_back(batch, carry)

    lax.fori_loop(1, batches, back, 0)
    for sent, got in ((sent_a, got_a), (sent_b, got_b)):
        pltpu.make_async_copy(sent.at[most], got.at[most], send_sem).wait()


def finish_body(tiles_h, latent, cells, latent_o, cells_o, tiles, tiles_sem, latent_sem, cells_sem):
    load = pltpu.make_async_copy(tiles_h, tiles, tiles_sem)
    load.start()
    whole = pltpu.make_async_copy(latent, latent_o, latent_sem)
    whole.start()
    load.wait()

    def place(s, carry):
        for half in range(2):
            to = pl.ds(pl.multiple_of(tiles[2 * s + half] * BC, BC), BC)
            rows = pl.ds(half * latent.shape[0], latent.shape[0])
            pltpu.make_async_copy(cells.at[s, rows], cells_o.at[:, to], cells_sem).start()
        return carry

    lax.fori_loop(0, cells.shape[0], place, 0, unroll=8)
    pltpu.make_async_copy(cells_o, cells_o, cells_sem).wait()
    whole.wait()


def shards(
    fields_a,
    latent_b,
    regrid_w,
    cell_tiles,
    norm_a,
    enc_in,
    enc_mid,
    enc_out,
    norm_b,
    dec_mid,
    dec_out,
):
    groups = lax.axis_size("ch")
    samples, nodes, hidden = latent_b.shape
    all_cells = fields_a.shape[2]
    bf16, f32 = jnp.bfloat16, jnp.float32
    tiles = cell_tiles.reshape(-1)
    fields = jnp.swapaxes(fields_a.reshape(samples // 8, 8, all_cells // BC, BC), 1, 2)
    regrid = jnp.swapaxes(regrid_w, 2, 3).reshape(groups, 2 * BN, BC)
    args = (
        tiles,
        fields,
        regrid,
        latent_b,
        norm_a,
        enc_in,
        enc_mid,
        enc_out,
        norm_b.reshape(1, -1),
        dec_mid,
        dec_out,
    )
    hbm = pl.BlockSpec(memory_space=pltpu.HBM)
    vmem = pl.BlockSpec(memory_space=pltpu.VMEM)
    message = pltpu.VMEM((groups, samples, nodes), bf16)
    latent_a, cells = pl.pallas_call(
        functools.partial(main_body, groups),
        out_shape=[
            pltpu.VMEM((samples, nodes, hidden), bf16),
            pltpu.VMEM((groups, 2 * samples, BC), bf16),
        ],
        in_specs=[hbm] * 11,
        out_specs=[vmem] * 2,
        scratch_shapes=[
            pltpu.SMEM(tiles.shape, jnp.int32),
            pltpu.SMEM(norm_a.shape, f32),
            pltpu.VMEM(fields.shape, bf16),
            pltpu.VMEM(regrid.shape, bf16),
            pltpu.VMEM(latent_b.shape, bf16),
            pltpu.VMEM(enc_in.shape, bf16),
            pltpu.VMEM(enc_mid.shape, bf16),
            pltpu.VMEM(enc_out.shape, bf16),
            pltpu.VMEM((1, hidden), f32),
            pltpu.VMEM(dec_mid.shape, bf16),
            pltpu.VMEM(dec_out.shape, bf16),
            message,
            message,
            message,
            message,
            pltpu.VMEM((groups * PITCH_A, nodes), f32),
            pltpu.VMEM((samples * PITCH_B, nodes), f32),
            pltpu.SemaphoreType.DMA((10,)),
            pltpu.SemaphoreType.DMA((groups // CHUNK,)),
            pltpu.SemaphoreType.DMA,
            pltpu.SemaphoreType.DMA,
            pltpu.SemaphoreType.DMA((groups // BATCH,)),
        ],
        compiler_params=pltpu.CompilerParams(
            collective_id=0, has_side_effects=True, vmem_limit_bytes=40 * 2**20
        ),
        name="main",
    )(*map(in_hbm, args))
    latent_a, cells_b = pl.pallas_call(
        finish_body,
        out_shape=[
            pltpu.HBM(latent_a.shape, bf16),
            pltpu.HBM((samples, all_cells), bf16),
        ],
        in_specs=[hbm, vmem, vmem],
        out_specs=[hbm, hbm],
        scratch_shapes=[
            pltpu.SMEM(tiles.shape, jnp.int32),
            pltpu.SemaphoreType.DMA,
            pltpu.SemaphoreType.DMA,
            pltpu.SemaphoreType.DMA,
        ],
        name="finish",
    )(in_hbm(tiles), in_vmem(latent_a), in_vmem(cells))
    return latent_a, cells_b.reshape(samples, 1, all_cells)


def solution(mesh):
    sharded = P("rep", "ch", None)
    return jax.shard_map(
        shards,
        mesh=mesh,
        in_specs=(sharded, sharded) + (P(),) * 9,
        out_specs=(sharded, sharded),
        check_vma=False,
    )
```

```python
import functools

import jax
import jax.numpy as jnp
from jax import lax
from jax.experimental import pallas as pl
from jax.experimental.pallas import tpu as pltpu
from jax.sharding import PartitionSpec as P

BN = 64
BC = 128
EPSILON = 1e-05
BATCH = 8
TOGETHER = 4
CHUNK = 16
PITCH_A = 24
PITCH_B = 136
NT = (((1,), (1,)), ((), ()))
MESH = pl.DeviceIdType.MESH


in_hbm = functools.partial(pltpu.with_memory_space_constraint, memory_space=pltpu.HBM)
in_vmem = functools.partial(pltpu.with_memory_space_constraint, memory_space=pltpu.VMEM)


def silu(v):
    half = 0.5 * v
    return half + half * jnp.tanh(half)


def main_body(
    groups,
    tiles_h,
    fields_h,
    regrid_h,
    latent_h,
    norm_a_h,
    enc_in_h,
    enc_mid_h,
    enc_out_h,
    norm_b_h,
    dec_mid_h,
    dec_out_h,
    latent_o,
    cells_o,
    tiles,
    norm_a,
    fields,
    regrid,
    latent,
    enc_in,
    enc_mid,
    enc_out,
    norm_b,
    dec_mid,
    dec_out,
    sent_a,
    sent_b,
    got_a,
    got_b,
    stage_a,
    stage_b,
    load_sem,
    regrid_sem,
    send_sem,
    recv_a,
    recv_b,
):
    me = lax.axis_index("ch")
    samples, nodes = latent.shape[:2]
    chunks = groups // CHUNK
    batches = groups // BATCH

    def load(k, src, dst):
        copy = pltpu.make_async_copy(src, dst, load_sem.at[k])
        copy.start()
        return copy

    load_tiles = load(0, tiles_h, tiles)
    load_fields = load(1, fields_h, fields)
    load_regrid = []
    for k in range(chunks):
        part = pl.ds(lax.rem(me // CHUNK + k, chunks) * CHUNK, CHUNK)
        copy = pltpu.make_async_copy(regrid_h.at[part], regrid.at[part], regrid_sem.at[k])
        copy.start()
        load_regrid.append(copy)
    load_dec = [
        load(2, latent_h, latent),
        load(3, norm_b_h, norm_b),
        load(4, dec_mid_h, dec_mid),
        load(5, dec_out_h, dec_out),
    ]
    load_enc = [
        load(6, norm_a_h, norm_a),
        load(7, enc_in_h, enc_in),
        load(8, enc_mid_h, enc_mid),
        load(9, enc_out_h, enc_out),
    ]

    barrier = pltpu.get_barrier_semaphore()

    def greet(step, carry):
        peer = {"ch": lax.rem(me + step, groups)}
        pl.semaphore_signal(barrier, inc=1, device_id=peer, device_id_type=MESH)
        return carry

    lax.fori_loop(1, groups, greet, 0, unroll=8)

    left_half = lax.broadcasted_iota(jnp.int32, (samples, BC), 1) < BN

    def send(sent, got, sem_of):
        def one(step, carry):
            peer = lax.rem(me + step, groups)
            pltpu.make_async_remote_copy(
                src_ref=sent.at[peer],
                dst_ref=got.at[me],
                send_sem=send_sem,
                recv_sem=sem_of(step),
                device_id={"ch": peer},
                device_id_type=MESH,
            ).start()
            return carry

        return one

    send_a = send(sent_a, got_a, lambda step: recv_a)
    send_b = send(sent_b, got_b, lambda step: recv_b.at[step // BATCH])

    def regrid_batch(batch):
        for j in range(BATCH):
            d = lax.rem(me + batch * BATCH + j, groups)
            blocks = [tiles[2 * d], tiles[2 * d + 1]]
            x = [fields[rows, block] for block in blocks for rows in range(fields.shape[0])]
            both = lax.dot_general(
                jnp.concatenate(x, axis=0), regrid[d], NT, preferred_element_type=jnp.float32
            )
            mine = jnp.where(left_half, both[:samples], both[samples:])
            sent_a[d] = mine.astype(jnp.bfloat16)

    load_tiles.wait()
    load_fields.wait()
    load_regrid[0].wait()
    ahead = batches // 4
    per_chunk = CHUNK // BATCH
    for batch in range(ahead):
        if batch % per_chunk == 0:
            load_regrid[batch // per_chunk + 1].wait()
        regrid_batch(batch)
    got_a[me] = sent_a[me]
    pl.semaphore_wait(barrier, groups - 1)
    sent = 0
    for batch in range(ahead, batches):
        if batch % per_chunk == 0 and batch // per_chunk + 1 < chunks:
            load_regrid[batch // per_chunk + 1].wait()
        regrid_batch(batch)
        ready = min(batch, sent + 2)
        lax.fori_loop(max(1, sent * BATCH), ready * BATCH, send_a, 0, unroll=True)
        sent = ready
    lax.fori_loop(sent * BATCH, groups, send_a, 0, unroll=True)

    for copy in load_dec:
        copy.wait()

    def decode(block, carry):
        first = block * TOGETHER
        v = latent[pl.ds(first, TOGETHER)].astype(jnp.float32).reshape(TOGETHER * nodes, -1)
        centred = v - jnp.mean(v, axis=1, keepdims=True)
        spread = jnp.mean(centred * centred, axis=1, keepdims=True)
        normed = (centred * lax.rsqrt(spread + EPSILON) * norm_b[...]).astype(jnp.bfloat16)
        middle = silu(jnp.dot(normed, dec_mid[...], preferred_element_type=jnp.float32))
        out = jnp.dot(
            middle.astype(jnp.bfloat16), dec_out[...], preferred_element_type=jnp.float32
        )
        for k in range(TOGETHER):
            rows = pl.ds(pl.multiple_of((first + k) * PITCH_B, 8), groups)
            stage_b[rows, :] = out[k * nodes : (k + 1) * nodes].T
        return carry

    lax.fori_loop(0, samples // TOGETHER, decode, 0)

    def pack_batch(batch, carry):
        for j in range(BATCH):
            c = lax.rem(me + batch * BATCH + j, groups)
            rows = stage_b[pl.ds(c, samples, stride=PITCH_B), :]
            sent_b[c] = rows.astype(jnp.bfloat16)
        return carry

    def pack_and_send(batch, carry):
        pack_batch(batch, carry)
        for j in range(BATCH):
            send_b((batch - 1) * BATCH + j, carry)
        return carry

    pack_batch(0, 0)
    pack_batch(1, 0)
    lax.fori_loop(1, BATCH, send_b, 0, unroll=True)
    lax.fori_loop(2, batches, pack_and_send, 0)
    lax.fori_loop(groups - BATCH, groups, send_b, 0, unroll=True)
    got_b[me] = sent_b[me]

    for copy in load_enc:
        copy.wait()
    most = pl.ds(0, groups - 1)
    pltpu.make_async_copy(sent_a.at[most], got_a.at[most], recv_a).wait()

    def add(c, total):
        return total + got_a[c].astype(jnp.float32)

    zero = jnp.zeros((samples, nodes), jnp.float32)
    average = lax.fori_loop(0, groups, add, zero, unroll=8) / groups

    def add_square(c, total):
        centred = got_a[c].astype(jnp.float32) - average
        return total + centred * centred

    spread = lax.fori_loop(0, groups, add_square, zero, unroll=8) / groups
    factor = lax.rsqrt(spread + EPSILON)

    def scale(c, carry):
        centred = got_a[c].astype(jnp.float32) - average
        rows = pl.ds(pl.multiple_of(c * PITCH_A, 8), samples)
        stage_a[rows, :] = centred * factor * norm_a[c]
        return carry

    lax.fori_loop(0, groups, scale, 0, unroll=8)

    def encode(block, carry):
        first = block * TOGETHER
        normed = jnp.concatenate(
            [stage_a[pl.ds(first + k, groups, stride=PITCH_A), :].T for k in range(TOGETHER)],
            axis=0,
        ).astype(jnp.bfloat16)
        base = jnp.dot(normed, enc_in[...], preferred_element_type=jnp.float32).astype(jnp.bfloat16)
        middle = silu(jnp.dot(base, enc_mid[...], preferred_element_type=jnp.float32))
        out = base.astype(jnp.float32) + jnp.dot(
            middle.astype(jnp.bfloat16), enc_out[...], preferred_element_type=jnp.float32
        )
        latent_o[pl.ds(first, TOGETHER)] = out.astype(jnp.bfloat16).reshape(TOGETHER, nodes, -1)
        return carry

    lax.fori_loop(0, samples // TOGETHER, encode, 0)

    def regrid_back(batch, carry):
        for j in range(BATCH):
            s = lax.rem(me + groups - batch * BATCH - j, groups)
            x = got_b[s]
            none = jnp.zeros_like(x)
            split = jnp.concatenate([jnp.where(left_half, x, none), jnp.where(left_half, none, x)], axis=0)
            cells = jnp.dot(split, regrid[s], preferred_element_type=jnp.float32)
            cells_o[s] = cells.astype(jnp.bfloat16)
        return carry

    def wait_back(batch, count):
        part = pl.ds(0, count)
        pltpu.make_async_copy(sent_b.at[part], got_b.at[part], recv_b.at[batch]).wait()

    wait_back(0, BATCH - 1)
    regrid_back(0, 0)

    def back(batch, carry):
        wait_back(batch, BATCH)
        return regrid_back(batch, carry)

    lax.fori_loop(1, batches, back, 0)
    for sent, got in ((sent_a, got_a), (sent_b, got_b)):
        pltpu.make_async_copy(sent.at[most], got.at[most], send_sem).wait()


def finish_body(tiles_h, latent, cells, latent_o, cells_o, tiles, tiles_sem, latent_sem, cells_sem):
    load = pltpu.make_async_copy(tiles_h, tiles, tiles_sem)
    load.start()
    whole = pltpu.make_async_copy(latent, latent_o, latent_sem)
    whole.start()
    load.wait()

    def place(s, carry):
        for half in range(2):
            to = pl.ds(pl.multiple_of(tiles[2 * s + half] * BC, BC), BC)
            rows = pl.ds(half * latent.shape[0], latent.shape[0])
            pltpu.make_async_copy(cells.at[s, rows], cells_o.at[:, to], cells_sem).start()
        return carry

    lax.fori_loop(0, cells.shape[0], place, 0, unroll=8)
    pltpu.make_async_copy(cells_o, cells_o, cells_sem).wait()
    whole.wait()


def shards(
    fields_a,
    latent_b,
    regrid_w,
    cell_tiles,
    norm_a,
    enc_in,
    enc_mid,
    enc_out,
    norm_b,
    dec_mid,
    dec_out,
):
    groups = lax.axis_size("ch")
    samples, nodes, hidden = latent_b.shape
    all_cells = fields_a.shape[2]
    bf16, f32 = jnp.bfloat16, jnp.float32
    tiles = cell_tiles.reshape(-1)
    fields = jnp.swapaxes(fields_a.reshape(samples // 8, 8, all_cells // BC, BC), 1, 2)
    regrid = jnp.swapaxes(regrid_w, 2, 3).reshape(groups, 2 * BN, BC)
    args = (
        tiles,
        fields,
        regrid,
        latent_b,
        norm_a,
        enc_in,
        enc_mid,
        enc_out,
        norm_b.reshape(1, -1),
        dec_mid,
        dec_out,
    )
    hbm = pl.BlockSpec(memory_space=pltpu.HBM)
    vmem = pl.BlockSpec(memory_space=pltpu.VMEM)
    message = pltpu.VMEM((groups, samples, nodes), bf16)
    latent_a, cells = pl.pallas_call(
        functools.partial(main_body, groups),
        out_shape=[
            pltpu.VMEM((samples, nodes, hidden), bf16),
            pltpu.VMEM((groups, 2 * samples, BC), bf16),
        ],
        in_specs=[hbm] * 11,
        out_specs=[vmem] * 2,
        scratch_shapes=[
            pltpu.SMEM(tiles.shape, jnp.int32),
            pltpu.SMEM(norm_a.shape, f32),
            pltpu.VMEM(fields.shape, bf16),
            pltpu.VMEM(regrid.shape, bf16),
            pltpu.VMEM(latent_b.shape, bf16),
            pltpu.VMEM(enc_in.shape, bf16),
            pltpu.VMEM(enc_mid.shape, bf16),
            pltpu.VMEM(enc_out.shape, bf16),
            pltpu.VMEM((1, hidden), f32),
            pltpu.VMEM(dec_mid.shape, bf16),
            pltpu.VMEM(dec_out.shape, bf16),
            message,
            message,
            message,
            message,
            pltpu.VMEM((groups * PITCH_A, nodes), f32),
            pltpu.VMEM((samples * PITCH_B, nodes), f32),
            pltpu.SemaphoreType.DMA((10,)),
            pltpu.SemaphoreType.DMA((groups // CHUNK,)),
            pltpu.SemaphoreType.DMA,
            pltpu.SemaphoreType.DMA,
            pltpu.SemaphoreType.DMA((groups // BATCH,)),
        ],
        compiler_params=pltpu.CompilerParams(
            collective_id=0, has_side_effects=True, vmem_limit_bytes=40 * 2**20
        ),
        name="main",
    )(*map(in_hbm, args))
    latent_a, cells_b = pl.pallas_call(
        finish_body,
        out_shape=[
            pltpu.HBM(latent_a.shape, bf16),
            pltpu.HBM((samples, all_cells), bf16),
        ],
        in_specs=[hbm, vmem, vmem],
        out_specs=[hbm, hbm],
        scratch_shapes=[
            pltpu.SMEM(tiles.shape, jnp.int32),
            pltpu.SemaphoreType.DMA,
            pltpu.SemaphoreType.DMA,
            pltpu.SemaphoreType.DMA,
        ],
        name="finish",
    )(in_hbm(tiles), in_vmem(latent_a), in_vmem(cells))
    return latent_a, cells_b.reshape(samples, 1, all_cells)


def solution(mesh):
    sharded = P("rep", "ch", None)
    return jax.shard_map(
        shards,
        mesh=mesh,
        in_specs=(sharded, sharded) + (P(),) * 9,
        out_specs=(sharded, sharded),
        check_vma=False,
    )
```

```python
import functools
import itertools

import jax
import jax.numpy as jnp
from jax import lax
from jax.experimental import pallas as pl
from jax.experimental.pallas import tpu as pltpu
from jax.sharding import PartitionSpec as P

BN = 64
BC = 128
EPSILON = 1e-05
BATCH = 8
TOGETHER = 4
CHUNK = 16
PITCH_A = 24
PITCH_B = 136
BOX = (4, 2, 8, 2)
WAYS = sorted(
    itertools.product(*map(range, BOX)),
    key=lambda way: -sum(min(k, size - k) for k, size in zip(way[:3], (4, 4, 8))),
)
NT = (((1,), (1,)), ((), ()))
MESH = pl.DeviceIdType.MESH


in_hbm = functools.partial(pltpu.with_memory_space_constraint, memory_space=pltpu.HBM)
in_vmem = functools.partial(pltpu.with_memory_space_constraint, memory_space=pltpu.VMEM)
in_smem = functools.partial(pltpu.with_memory_space_constraint, memory_space=pltpu.SMEM)


def silu(v):
    half = 0.5 * v
    return half + half * jnp.tanh(half)


def main_body(
    groups,
    tiles_h,
    fields_h,
    regrid_h,
    latent_h,
    norm_a_h,
    enc_in_h,
    enc_mid_h,
    enc_out_h,
    norm_b_h,
    dec_mid_h,
    dec_out_h,
    latent_o,
    cells_o,
    tiles,
    norm_a,
    fields,
    regrid,
    latent,
    enc_in,
    enc_mid,
    enc_out,
    norm_b,
    dec_mid,
    dec_out,
    sent_a,
    sent_b,
    got_a,
    got_b,
    stage_a,
    stage_b,
    load_sem,
    regrid_sem,
    send_sem,
    recv_a,
    recv_b,
):
    me = lax.axis_index("ch")
    samples, nodes = latent.shape[:2]
    chunks = groups // CHUNK
    batches = groups // BATCH

    def load(k, src, dst):
        copy = pltpu.make_async_copy(src, dst, load_sem.at[k])
        copy.start()
        return copy

    load_tiles = load(0, tiles_h, tiles)
    load_fields = load(1, fields_h, fields)
    load_regrid = []
    for k in range(chunks):
        part = pl.ds(lax.rem(me // CHUNK + k, chunks) * CHUNK, CHUNK)
        copy = pltpu.make_async_copy(regrid_h.at[part], regrid.at[part], regrid_sem.at[k])
        copy.start()
        load_regrid.append(copy)
    load_dec = [
        load(2, latent_h, latent),
        load(3, norm_b_h, norm_b),
        load(4, dec_mid_h, dec_mid),
        load(5, dec_out_h, dec_out),
    ]
    load_enc = [
        load(6, norm_a_h, norm_a),
        load(7, enc_in_h, enc_in),
        load(8, enc_mid_h, enc_mid),
        load(9, enc_out_h, enc_out),
    ]

    barrier = pltpu.get_barrier_semaphore()

    x, y = me // (groups // BOX[0]), lax.rem(me // (BOX[2] * BOX[3]), BOX[1])
    z, core = lax.rem(me // BOX[3], BOX[2]), lax.rem(me, BOX[3])
    place, step = (x, y, z, core), (groups // BOX[0], BOX[2] * BOX[3], BOX[3], 1)
    parts = [
        [lax.rem(place[axis] + k, BOX[axis]) * step[axis] for k in range(BOX[axis])]
        for axis in range(4)
    ]
    planes = [[first + second for second in parts[1]] for first in parts[0]]
    lines = [[first + second for second in parts[3]] for first in parts[2]]
    for dx, dy, dz, dc in WAYS:
        if dx or dy or dz or dc:
            peer = {"ch": planes[dx][dy] + lines[dz][dc]}
            pl.semaphore_signal(barrier, inc=1, device_id=peer, device_id_type=MESH)

    left_half = lax.broadcasted_iota(jnp.int32, (samples, BC), 1) < BN

    def send(sent, got, sem_of):
        def one(step, carry):
            peer = lax.rem(me + step, groups)
            pltpu.make_async_remote_copy(
                src_ref=sent.at[peer],
                dst_ref=got.at[me],
                send_sem=send_sem,
                recv_sem=sem_of(step),
                device_id={"ch": peer},
                device_id_type=MESH,
            ).start()
            return carry

        return one

    send_a = send(sent_a, got_a, lambda step: recv_a)
    send_b = send(sent_b, got_b, lambda step: recv_b.at[step // BATCH])

    def regrid_batch(batch):
        for j in range(BATCH):
            d = lax.rem(me + batch * BATCH + j, groups)
            blocks = [tiles[2 * d], tiles[2 * d + 1]]
            x = [fields[rows, block] for block in blocks for rows in range(fields.shape[0])]
            both = lax.dot_general(
                jnp.concatenate(x, axis=0), regrid[d], NT, preferred_element_type=jnp.float32
            )
            mine = jnp.where(left_half, both[:samples], both[samples:])
            sent_a[d] = mine.astype(jnp.bfloat16)

    load_tiles.wait()
    load_fields.wait()
    load_regrid[0].wait()
    ahead = batches // 4
    per_chunk = CHUNK // BATCH
    for batch in range(ahead):
        if batch % per_chunk == 0:
            load_regrid[batch // per_chunk + 1].wait()
        regrid_batch(batch)
    got_a[me] = sent_a[me]
    pl.semaphore_wait(barrier, groups - 1)
    sent = 0
    for batch in range(ahead, batches):
        if batch % per_chunk == 0 and batch // per_chunk + 1 < chunks:
            load_regrid[batch // per_chunk + 1].wait()
        regrid_batch(batch)
        ready = min(batch, sent + 2)
        lax.fori_loop(max(1, sent * BATCH), ready * BATCH, send_a, 0, unroll=True)
        sent = ready
    lax.fori_loop(sent * BATCH, groups, send_a, 0, unroll=True)

    for copy in load_dec:
        copy.wait()

    def decode(block, carry):
        first = block * TOGETHER
        v = latent[pl.ds(first, TOGETHER)].astype(jnp.float32).reshape(TOGETHER * nodes, -1)
        centred = v - jnp.mean(v, axis=1, keepdims=True)
        spread = jnp.mean(centred * centred, axis=1, keepdims=True)
        normed = (centred * lax.rsqrt(spread + EPSILON) * norm_b[...]).astype(jnp.bfloat16)
        middle = silu(jnp.dot(normed, dec_mid[...], preferred_element_type=jnp.float32))
        out = jnp.dot(
            middle.astype(jnp.bfloat16), dec_out[...], preferred_element_type=jnp.float32
        )
        for k in range(TOGETHER):
            rows = pl.ds(pl.multiple_of((first + k) * PITCH_B, 8), groups)
            stage_b[rows, :] = out[k * nodes : (k + 1) * nodes].T
        return carry

    lax.fori_loop(0, samples // TOGETHER, decode, 0)

    def pack_batch(batch, carry):
        for j in range(BATCH):
            c = lax.rem(me + batch * BATCH + j, groups)
            rows = stage_b[pl.ds(c, samples, stride=PITCH_B), :]
            sent_b[c] = rows.astype(jnp.bfloat16)
        return carry

    def pack_and_send(batch, carry):
        pack_batch(batch, carry)
        for j in range(BATCH):
            send_b((batch - 1) * BATCH + j, carry)
        return carry

    pack_batch(0, 0)
    pack_batch(1, 0)
    lax.fori_loop(1, BATCH, send_b, 0, unroll=True)
    lax.fori_loop(2, batches, pack_and_send, 0)
    lax.fori_loop(groups - BATCH, groups, send_b, 0, unroll=True)
    got_b[me] = sent_b[me]

    for copy in load_enc:
        copy.wait()
    most = pl.ds(0, groups - 1)
    pltpu.make_async_copy(sent_a.at[most], got_a.at[most], recv_a).wait()

    def add(c, total):
        return total + got_a[c].astype(jnp.float32)

    zero = jnp.zeros((samples, nodes), jnp.float32)
    average = lax.fori_loop(0, groups, add, zero, unroll=8) / groups

    def add_square(c, total):
        centred = got_a[c].astype(jnp.float32) - average
        return total + centred * centred

    spread = lax.fori_loop(0, groups, add_square, zero, unroll=8) / groups
    factor = lax.rsqrt(spread + EPSILON)

    def scale(c, carry):
        centred = got_a[c].astype(jnp.float32) - average
        rows = pl.ds(pl.multiple_of(c * PITCH_A, 8), samples)
        stage_a[rows, :] = centred * factor * norm_a[c]
        return carry

    lax.fori_loop(0, groups, scale, 0, unroll=8)

    def encode(block, carry):
        first = block * TOGETHER
        normed = jnp.concatenate(
            [stage_a[pl.ds(first + k, groups, stride=PITCH_A), :].T for k in range(TOGETHER)],
            axis=0,
        ).astype(jnp.bfloat16)
        base = jnp.dot(normed, enc_in[...], preferred_element_type=jnp.float32).astype(jnp.bfloat16)
        middle = silu(jnp.dot(base, enc_mid[...], preferred_element_type=jnp.float32))
        out = base.astype(jnp.float32) + jnp.dot(
            middle.astype(jnp.bfloat16), enc_out[...], preferred_element_type=jnp.float32
        )
        latent_o[pl.ds(first, TOGETHER)] = out.astype(jnp.bfloat16).reshape(TOGETHER, nodes, -1)
        return carry

    lax.fori_loop(0, samples // TOGETHER, encode, 0)

    def regrid_back(batch, carry):
        for j in range(BATCH):
            s = lax.rem(me + groups - batch * BATCH - j, groups)
            x = got_b[s]
            none = jnp.zeros_like(x)
            split = jnp.concatenate([jnp.where(left_half, x, none), jnp.where(left_half, none, x)], axis=0)
            cells = jnp.dot(split, regrid[s], preferred_element_type=jnp.float32)
            cells_o[s] = cells.astype(jnp.bfloat16)
        return carry

    def wait_back(batch, count):
        part = pl.ds(0, count)
        pltpu.make_async_copy(sent_b.at[part], got_b.at[part], recv_b.at[batch]).wait()

    wait_back(0, BATCH - 1)
    regrid_back(0, 0)

    def back(batch, carry):
        wait_back(batch, BATCH)
        return regrid_back(batch, carry)

    lax.fori_loop(1, batches, back, 0)
    for sent, got in ((sent_a, got_a), (sent_b, got_b)):
        pltpu.make_async_copy(sent.at[most], got.at[most], send_sem).wait()


def finish_body(tiles, latent, cells, latent_o, cells_o, placed, sem):
    copies = [pltpu.make_async_copy(latent, latent_o, sem.at[0])]
    copies[0].start()
    parts, rows = placed.shape[0], placed.shape[2]

    def place(s, carry):
        for half in range(2):
            to = tiles[2 * s + half]
            for part in range(parts):
                first = (half * parts + part) * rows
                placed[part, to] = cells[s, first : first + rows]
        return carry

    lax.fori_loop(0, cells.shape[0], place, 0, unroll=8)
    copies.append(pltpu.make_async_copy(placed, cells_o, sem.at[1]))
    copies[1].start()
    for copy in copies:
        copy.wait()


def shards(
    fields_a,
    latent_b,
    regrid_w,
    cell_tiles,
    norm_a,
    enc_in,
    enc_mid,
    enc_out,
    norm_b,
    dec_mid,
    dec_out,
):
    groups = lax.axis_size("ch")
    samples, nodes, hidden = latent_b.shape
    all_cells = fields_a.shape[2]
    bf16, f32 = jnp.bfloat16, jnp.float32
    tiles = cell_tiles.reshape(-1)
    fields = jnp.swapaxes(fields_a.reshape(samples // 8, 8, all_cells // BC, BC), 1, 2)
    regrid = jnp.swapaxes(regrid_w, 2, 3).reshape(groups, 2 * BN, BC)
    args = (
        tiles,
        fields,
        regrid,
        latent_b,
        norm_a,
        enc_in,
        enc_mid,
        enc_out,
        norm_b.reshape(1, -1),
        dec_mid,
        dec_out,
    )
    hbm = pl.BlockSpec(memory_space=pltpu.HBM)
    vmem = pl.BlockSpec(memory_space=pltpu.VMEM)
    smem = pl.BlockSpec(memory_space=pltpu.SMEM)
    message = pltpu.VMEM((groups, samples, nodes), bf16)
    latent_a, cells, tiles = pl.pallas_call(
        functools.partial(main_body, groups),
        out_shape=[
            pltpu.VMEM((samples, nodes, hidden), bf16),
            pltpu.VMEM((groups, 2 * samples, BC), bf16),
            pltpu.SMEM(tiles.shape, jnp.int32),
        ],
        in_specs=[hbm] * 11,
        out_specs=[vmem, vmem, smem],
        scratch_shapes=[
            pltpu.SMEM(norm_a.shape, f32),
            pltpu.VMEM(fields.shape, bf16),
            pltpu.VMEM(regrid.shape, bf16),
            pltpu.VMEM(latent_b.shape, bf16),
            pltpu.VMEM(enc_in.shape, bf16),
            pltpu.VMEM(enc_mid.shape, bf16),
            pltpu.VMEM(enc_out.shape, bf16),
            pltpu.VMEM((1, hidden), f32),
            pltpu.VMEM(dec_mid.shape, bf16),
            pltpu.VMEM(dec_out.shape, bf16),
            message,
            message,
            message,
            message,
            pltpu.VMEM((groups * PITCH_A, nodes), f32),
            pltpu.VMEM((samples * PITCH_B, nodes), f32),
            pltpu.SemaphoreType.DMA((10,)),
            pltpu.SemaphoreType.DMA((groups // CHUNK,)),
            pltpu.SemaphoreType.DMA,
            pltpu.SemaphoreType.DMA,
            pltpu.SemaphoreType.DMA((groups // BATCH,)),
        ],
        compiler_params=pltpu.CompilerParams(
            collective_id=0, has_side_effects=True, vmem_limit_bytes=40 * 2**20
        ),
        name="main",
    )(*map(in_hbm, args))
    latent_a, cells_b = pl.pallas_call(
        finish_body,
        out_shape=[
            pltpu.HBM(latent_a.shape, bf16),
            pltpu.HBM(fields.shape, bf16),
        ],
        in_specs=[smem, vmem, vmem],
        out_specs=[hbm, hbm],
        scratch_shapes=[
            pltpu.VMEM(fields.shape, bf16),
            pltpu.SemaphoreType.DMA((2,)),
        ],
        name="finish",
    )(in_smem(tiles), in_vmem(latent_a), in_vmem(cells))
    return latent_a, jnp.swapaxes(cells_b, 1, 2).reshape(samples, 1, all_cells)


def solution(mesh):
    sharded = P("rep", "ch", None)
    return jax.shard_map(
        shards,
        mesh=mesh,
        in_specs=(sharded, sharded) + (P(),) * 9,
        out_specs=(sharded, sharded),
        check_vma=False,
    )
```

```python
import functools
import itertools

import jax
import jax.numpy as jnp
from jax import lax
from jax.experimental import pallas as pl
from jax.experimental.pallas import tpu as pltpu
from jax.sharding import PartitionSpec as P

BN = 64
BC = 128
EPSILON = 1e-05
BATCH = 8
TOGETHER = 4
CHUNK = 16
EARLY = 1
PITCH_A = 24
PITCH_B = 136
BOX = (4, 2, 8, 2)
WAYS = sorted(
    itertools.product(*map(range, BOX)),
    key=lambda way: -sum(min(k, size - k) for k, size in zip(way[:3], (4, 4, 8))),
)
NT = (((1,), (1,)), ((), ()))
MESH = pl.DeviceIdType.MESH


in_hbm = functools.partial(pltpu.with_memory_space_constraint, memory_space=pltpu.HBM)
in_vmem = functools.partial(pltpu.with_memory_space_constraint, memory_space=pltpu.VMEM)
in_smem = functools.partial(pltpu.with_memory_space_constraint, memory_space=pltpu.SMEM)


def silu(v):
    half = 0.5 * v
    return half + half * jnp.tanh(half)


def main_body(
    groups,
    tiles_h,
    fields_h,
    regrid_h,
    latent_h,
    norm_a_h,
    enc_in_h,
    enc_mid_h,
    enc_out_h,
    norm_b_h,
    dec_mid_h,
    dec_out_h,
    latent_o,
    cells_o,
    tiles,
    norm_a,
    fields,
    regrid,
    latent,
    enc_in,
    enc_mid,
    enc_out,
    norm_b,
    dec_mid,
    dec_out,
    sent_a,
    sent_b,
    early_b,
    got_a,
    got_b,
    stage_a,
    stage_b,
    load_sem,
    regrid_sem,
    send_sem,
    recv_a,
    recv_b,
):
    me = lax.axis_index("ch")
    samples, nodes = latent.shape[:2]
    chunks = groups // CHUNK
    batches = groups // BATCH

    def load(k, src, dst):
        copy = pltpu.make_async_copy(src, dst, load_sem.at[k])
        copy.start()
        return copy

    load_tiles = load(0, tiles_h, tiles)
    load_fields = load(1, fields_h, fields)
    load_regrid = []
    for k in range(chunks):
        part = pl.ds(lax.rem(me // CHUNK + k, chunks) * CHUNK, CHUNK)
        copy = pltpu.make_async_copy(regrid_h.at[part], regrid.at[part], regrid_sem.at[k])
        copy.start()
        load_regrid.append(copy)
    load_dec = [
        load(2, latent_h, latent),
        load(3, norm_b_h, norm_b),
        load(4, dec_mid_h, dec_mid),
        load(5, dec_out_h, dec_out),
    ]
    load_enc = [
        load(6, norm_a_h, norm_a),
        load(7, enc_in_h, enc_in),
        load(8, enc_mid_h, enc_mid),
        load(9, enc_out_h, enc_out),
    ]

    barrier = pltpu.get_barrier_semaphore()

    x, y = me // (groups // BOX[0]), lax.rem(me // (BOX[2] * BOX[3]), BOX[1])
    z, core = lax.rem(me // BOX[3], BOX[2]), lax.rem(me, BOX[3])
    place, step = (x, y, z, core), (groups // BOX[0], BOX[2] * BOX[3], BOX[3], 1)
    parts = [
        [lax.rem(place[axis] + k, BOX[axis]) * step[axis] for k in range(BOX[axis])]
        for axis in range(4)
    ]
    planes = [[first + second for second in parts[1]] for first in parts[0]]
    lines = [[first + second for second in parts[3]] for first in parts[2]]
    for dx, dy, dz, dc in WAYS:
        if dx or dy or dz or dc:
            peer = {"ch": planes[dx][dy] + lines[dz][dc]}
            pl.semaphore_signal(barrier, inc=1, device_id=peer, device_id_type=MESH)

    left_half = lax.broadcasted_iota(jnp.int32, (samples, BC), 1) < BN

    def send(sent, got, sem_of):
        def one(step, carry):
            peer = lax.rem(me + step, groups)
            pltpu.make_async_remote_copy(
                src_ref=sent.at[peer],
                dst_ref=got.at[me],
                send_sem=send_sem,
                recv_sem=sem_of(step),
                device_id={"ch": peer},
                device_id_type=MESH,
            ).start()
            return carry

        return one

    send_a = send(sent_a, got_a, lambda step: recv_a)
    def copy_b(src, peer, step):
        pltpu.make_async_remote_copy(
            src_ref=src,
            dst_ref=got_b.at[me],
            send_sem=send_sem,
            recv_sem=recv_b.at[step // BATCH],
            device_id={"ch": peer},
            device_id_type=MESH,
        ).start()

    def send_b(step, carry):
        peer = lax.rem(me + step, groups)

        @pl.when(lax.rem(peer // BOX[3], BOX[2]) >= EARLY)
        def _():
            copy_b(sent_b.at[peer], peer, step)

        return carry

    per_layer = groups // BOX[2]
    place_in_layer = me // (BOX[2] * BOX[3]) * BOX[3] + core

    def early(k):
        there = lax.rem(place_in_layer + k % per_layer, per_layer)
        layer = k // per_layer
        return (there // BOX[3] * BOX[2] + layer) * BOX[3] + lax.rem(there, BOX[3])

    def pack_early(batch):
        for k in range(batch * BATCH, (batch + 1) * BATCH):
            rows = stage_b[pl.ds(early(k), samples, stride=PITCH_B), :]
            early_b[k] = rows.astype(jnp.bfloat16)

    def send_early(batch):
        for k in range(batch * BATCH, (batch + 1) * BATCH):
            peer = early(k)

            @pl.when(peer != me)
            def _(k=k, peer=peer):
                copy_b(early_b.at[k], peer, lax.rem(peer + groups - me, groups))

    def regrid_batch(batch):
        for j in range(BATCH):
            d = lax.rem(me + batch * BATCH + j, groups)
            blocks = [tiles[2 * d], tiles[2 * d + 1]]
            x = [fields[rows, block] for block in blocks for rows in range(fields.shape[0])]
            both = lax.dot_general(
                jnp.concatenate(x, axis=0), regrid[d], NT, preferred_element_type=jnp.float32
            )
            mine = jnp.where(left_half, both[:samples], both[samples:])
            sent_a[d] = mine.astype(jnp.bfloat16)

    load_tiles.wait()
    load_fields.wait()
    load_regrid[0].wait()
    ahead = batches // 4
    per_chunk = CHUNK // BATCH
    for batch in range(ahead):
        if batch % per_chunk == 0:
            load_regrid[batch // per_chunk + 1].wait()
        regrid_batch(batch)
    got_a[me] = sent_a[me]
    pl.semaphore_wait(barrier, groups - 1)
    sent = 0
    for batch in range(ahead, batches):
        if batch % per_chunk == 0 and batch // per_chunk + 1 < chunks:
            load_regrid[batch // per_chunk + 1].wait()
        regrid_batch(batch)
        ready = min(batch, sent + 2)
        lax.fori_loop(max(1, sent * BATCH), ready * BATCH, send_a, 0, unroll=True)
        sent = ready
    lax.fori_loop(sent * BATCH, groups, send_a, 0, unroll=True)

    for copy in load_dec:
        copy.wait()

    def decode(block, carry):
        first = block * TOGETHER
        v = latent[pl.ds(first, TOGETHER)].astype(jnp.float32).reshape(TOGETHER * nodes, -1)
        centred = v - jnp.mean(v, axis=1, keepdims=True)
        spread = jnp.mean(centred * centred, axis=1, keepdims=True)
        normed = (centred * lax.rsqrt(spread + EPSILON) * norm_b[...]).astype(jnp.bfloat16)
        middle = silu(jnp.dot(normed, dec_mid[...], preferred_element_type=jnp.float32))
        out = jnp.dot(
            middle.astype(jnp.bfloat16), dec_out[...], preferred_element_type=jnp.float32
        )
        for k in range(TOGETHER):
            rows = pl.ds(pl.multiple_of((first + k) * PITCH_B, 8), groups)
            stage_b[rows, :] = out[k * nodes : (k + 1) * nodes].T
        return carry

    lax.fori_loop(0, samples // TOGETHER, decode, 0)

    def pack_batch(batch, carry):
        for j in range(BATCH):
            c = lax.rem(me + batch * BATCH + j, groups)
            rows = stage_b[pl.ds(c, samples, stride=PITCH_B), :]
            sent_b[c] = rows.astype(jnp.bfloat16)
        return carry

    def pack_and_send(batch, carry):
        pack_batch(batch, carry)
        for j in range(BATCH):
            send_b((batch - 1) * BATCH + j, carry)
        return carry

    early_batches = EARLY * per_layer // BATCH
    pack_early(0)
    for batch in range(1, early_batches):
        pack_early(batch)
        send_early(batch - 1)
    pack_batch(0, 0)
    send_early(early_batches - 1)
    pack_batch(1, 0)
    lax.fori_loop(1, BATCH, send_b, 0, unroll=True)
    lax.fori_loop(2, batches, pack_and_send, 0)
    lax.fori_loop(groups - BATCH, groups, send_b, 0, unroll=True)
    got_b[me] = sent_b[me]

    for copy in load_enc:
        copy.wait()
    most = pl.ds(0, groups - 1)
    pltpu.make_async_copy(sent_a.at[most], got_a.at[most], recv_a).wait()

    def add(c, total):
        return total + got_a[c].astype(jnp.float32)

    zero = jnp.zeros((samples, nodes), jnp.float32)
    average = lax.fori_loop(0, groups, add, zero, unroll=8) / groups

    def add_square(c, total):
        centred = got_a[c].astype(jnp.float32) - average
        return total + centred * centred

    spread = lax.fori_loop(0, groups, add_square, zero, unroll=8) / groups
    factor = lax.rsqrt(spread + EPSILON)

    def scale(c, carry):
        centred = got_a[c].astype(jnp.float32) - average
        rows = pl.ds(pl.multiple_of(c * PITCH_A, 8), samples)
        stage_a[rows, :] = centred * factor * norm_a[c]
        return carry

    lax.fori_loop(0, groups, scale, 0, unroll=8)

    def encode(block, carry):
        first = block * TOGETHER
        normed = jnp.concatenate(
            [stage_a[pl.ds(first + k, groups, stride=PITCH_A), :].T for k in range(TOGETHER)],
            axis=0,
        ).astype(jnp.bfloat16)
        base = jnp.dot(normed, enc_in[...], preferred_element_type=jnp.float32).astype(jnp.bfloat16)
        middle = silu(jnp.dot(base, enc_mid[...], preferred_element_type=jnp.float32))
        out = base.astype(jnp.float32) + jnp.dot(
            middle.astype(jnp.bfloat16), enc_out[...], preferred_element_type=jnp.float32
        )
        latent_o[pl.ds(first, TOGETHER)] = out.astype(jnp.bfloat16).reshape(TOGETHER, nodes, -1)
        return carry

    lax.fori_loop(0, samples // TOGETHER, encode, 0)

    def regrid_back(batch, carry):
        for j in range(BATCH):
            s = lax.rem(me + groups - batch * BATCH - j, groups)
            x = got_b[s]
            none = jnp.zeros_like(x)
            split = jnp.concatenate([jnp.where(left_half, x, none), jnp.where(left_half, none, x)], axis=0)
            cells = jnp.dot(split, regrid[s], preferred_element_type=jnp.float32)
            cells_o[s] = cells.astype(jnp.bfloat16)
        return carry

    def wait_back(batch, count):
        part = pl.ds(0, count)
        pltpu.make_async_copy(sent_b.at[part], got_b.at[part], recv_b.at[batch]).wait()

    wait_back(0, BATCH - 1)
    regrid_back(0, 0)

    def back(batch, carry):
        wait_back(batch, BATCH)
        return regrid_back(batch, carry)

    lax.fori_loop(1, batches, back, 0)
    for sent, got in ((sent_a, got_a), (sent_b, got_b)):
        pltpu.make_async_copy(sent.at[most], got.at[most], send_sem).wait()


def finish_body(tiles, latent, cells, latent_o, cells_o, placed, sem):
    copies = [pltpu.make_async_copy(latent, latent_o, sem.at[0])]
    copies[0].start()
    parts, rows = placed.shape[0], placed.shape[2]

    def place(s, carry):
        for half in range(2):
            to = tiles[2 * s + half]
            for part in range(parts):
                first = (half * parts + part) * rows
                placed[part, to] = cells[s, first : first + rows]
        return carry

    lax.fori_loop(0, cells.shape[0], place, 0, unroll=8)
    copies.append(pltpu.make_async_copy(placed, cells_o, sem.at[1]))
    copies[1].start()
    for copy in copies:
        copy.wait()


def shards(
    fields_a,
    latent_b,
    regrid_w,
    cell_tiles,
    norm_a,
    enc_in,
    enc_mid,
    enc_out,
    norm_b,
    dec_mid,
    dec_out,
):
    groups = lax.axis_size("ch")
    samples, nodes, hidden = latent_b.shape
    all_cells = fields_a.shape[2]
    bf16, f32 = jnp.bfloat16, jnp.float32
    tiles = cell_tiles.reshape(-1)
    fields = jnp.swapaxes(fields_a.reshape(samples // 8, 8, all_cells // BC, BC), 1, 2)
    regrid = jnp.swapaxes(regrid_w, 2, 3).reshape(groups, 2 * BN, BC)
    args = (
        tiles,
        fields,
        regrid,
        latent_b,
        norm_a,
        enc_in,
        enc_mid,
        enc_out,
        norm_b.reshape(1, -1),
        dec_mid,
        dec_out,
    )
    hbm = pl.BlockSpec(memory_space=pltpu.HBM)
    vmem = pl.BlockSpec(memory_space=pltpu.VMEM)
    smem = pl.BlockSpec(memory_space=pltpu.SMEM)
    message = pltpu.VMEM((groups, samples, nodes), bf16)
    latent_a, cells, tiles = pl.pallas_call(
        functools.partial(main_body, groups),
        out_shape=[
            pltpu.VMEM((samples, nodes, hidden), bf16),
            pltpu.VMEM((groups, 2 * samples, BC), bf16),
            pltpu.SMEM(tiles.shape, jnp.int32),
        ],
        in_specs=[hbm] * 11,
        out_specs=[vmem, vmem, smem],
        scratch_shapes=[
            pltpu.SMEM(norm_a.shape, f32),
            pltpu.VMEM(fields.shape, bf16),
            pltpu.VMEM(regrid.shape, bf16),
            pltpu.VMEM(latent_b.shape, bf16),
            pltpu.VMEM(enc_in.shape, bf16),
            pltpu.VMEM(enc_mid.shape, bf16),
            pltpu.VMEM(enc_out.shape, bf16),
            pltpu.VMEM((1, hidden), f32),
            pltpu.VMEM(dec_mid.shape, bf16),
            pltpu.VMEM(dec_out.shape, bf16),
            message,
            message,
            pltpu.VMEM((EARLY * groups // BOX[2], samples, nodes), bf16),
            message,
            message,
            pltpu.VMEM((groups * PITCH_A, nodes), f32),
            pltpu.VMEM((samples * PITCH_B, nodes), f32),
            pltpu.SemaphoreType.DMA((10,)),
            pltpu.SemaphoreType.DMA((groups // CHUNK,)),
            pltpu.SemaphoreType.DMA,
            pltpu.SemaphoreType.DMA,
            pltpu.SemaphoreType.DMA((groups // BATCH,)),
        ],
        compiler_params=pltpu.CompilerParams(
            collective_id=0, has_side_effects=True, vmem_limit_bytes=40 * 2**20
        ),
        name="main",
    )(*map(in_hbm, args))
    latent_a, cells_b = pl.pallas_call(
        finish_body,
        out_shape=[
            pltpu.HBM(latent_a.shape, bf16),
            pltpu.HBM(fields.shape, bf16),
        ],
        in_specs=[smem, vmem, vmem],
        out_specs=[hbm, hbm],
        scratch_shapes=[
            pltpu.VMEM(fields.shape, bf16),
            pltpu.SemaphoreType.DMA((2,)),
        ],
        name="finish",
    )(in_smem(tiles), in_vmem(latent_a), in_vmem(cells))
    return latent_a, jnp.swapaxes(cells_b, 1, 2).reshape(samples, 1, all_cells)


def solution(mesh):
    sharded = P("rep", "ch", None)
    return jax.shard_map(
        shards,
        mesh=mesh,
        in_specs=(sharded, sharded) + (P(),) * 9,
        out_specs=(sharded, sharded),
        check_vma=False,
    )
```

```python
import functools
import itertools

import jax
import jax.numpy as jnp
from jax import lax
from jax.experimental import pallas as pl
from jax.experimental.pallas import tpu as pltpu
from jax.sharding import PartitionSpec as P

BN = 64
BC = 128
EPSILON = 1e-05
BATCH = 8
TOGETHER = 4
CHUNK = 16
EARLY = 1
PITCH_A = 24
PITCH_B = 136
BOX = (4, 2, 8, 2)
WAYS = sorted(
    itertools.product(*map(range, BOX)),
    key=lambda way: -sum(min(k, size - k) for k, size in zip(way[:3], (4, 4, 8))),
)
NT = (((1,), (1,)), ((), ()))
MESH = pl.DeviceIdType.MESH


in_hbm = functools.partial(pltpu.with_memory_space_constraint, memory_space=pltpu.HBM)
in_vmem = functools.partial(pltpu.with_memory_space_constraint, memory_space=pltpu.VMEM)
in_smem = functools.partial(pltpu.with_memory_space_constraint, memory_space=pltpu.SMEM)


def silu(v):
    half = 0.5 * v
    return half + half * jnp.tanh(half)


def main_body(
    groups,
    tiles_h,
    fields_h,
    regrid_h,
    latent_h,
    norm_a_h,
    enc_in_h,
    enc_mid_h,
    enc_out_h,
    norm_b_h,
    dec_mid_h,
    dec_out_h,
    latent_o,
    cells_o,
    tiles,
    norm_a,
    fields,
    regrid,
    latent,
    enc_in,
    enc_mid,
    enc_out,
    norm_b,
    dec_mid,
    dec_out,
    sent_a,
    sent_b,
    early_b,
    got_a,
    got_b,
    stage_a,
    stage_b,
    load_sem,
    regrid_sem,
    send_sem,
    recv_a,
    recv_b,
):
    me = lax.axis_index("ch")
    samples, nodes = latent.shape[:2]
    chunks = groups // CHUNK
    batches = groups // BATCH

    def load(k, src, dst):
        copy = pltpu.make_async_copy(src, dst, load_sem.at[k])
        copy.start()
        return copy

    load_tiles = load(0, tiles_h, tiles)
    load_fields = load(1, fields_h, fields)
    load_regrid = []
    for k in range(chunks):
        part = pl.ds(lax.rem(me // CHUNK + k, chunks) * CHUNK, CHUNK)
        copy = pltpu.make_async_copy(regrid_h.at[part], regrid.at[part], regrid_sem.at[k])
        copy.start()
        load_regrid.append(copy)
    load_dec = [
        load(2, latent_h, latent),
        load(3, norm_b_h, norm_b),
        load(4, dec_mid_h, dec_mid),
        load(5, dec_out_h, dec_out),
    ]
    load_enc = [
        load(6, norm_a_h, norm_a),
        load(7, enc_in_h, enc_in),
        load(8, enc_mid_h, enc_mid),
        load(9, enc_out_h, enc_out),
    ]

    barrier = pltpu.get_barrier_semaphore()

    x, y = me // (groups // BOX[0]), lax.rem(me // (BOX[2] * BOX[3]), BOX[1])
    z, core = lax.rem(me // BOX[3], BOX[2]), lax.rem(me, BOX[3])
    place, step = (x, y, z, core), (groups // BOX[0], BOX[2] * BOX[3], BOX[3], 1)
    parts = [
        [lax.rem(place[axis] + k, BOX[axis]) * step[axis] for k in range(BOX[axis])]
        for axis in range(4)
    ]
    planes = [[first + second for second in parts[1]] for first in parts[0]]
    lines = [[first + second for second in parts[3]] for first in parts[2]]
    for dx, dy, dz, dc in WAYS:
        if dx or dy or dz or dc:
            peer = {"ch": planes[dx][dy] + lines[dz][dc]}
            pl.semaphore_signal(barrier, inc=1, device_id=peer, device_id_type=MESH)

    left_half = lax.broadcasted_iota(jnp.int32, (samples, BC), 1) < BN

    def send(sent, got, sem_of):
        def one(step, carry):
            peer = lax.rem(me + step, groups)
            pltpu.make_async_remote_copy(
                src_ref=sent.at[peer],
                dst_ref=got.at[me],
                send_sem=send_sem,
                recv_sem=sem_of(step),
                device_id={"ch": peer},
                device_id_type=MESH,
            ).start()
            return carry

        return one

    send_a = send(sent_a, got_a, lambda step: recv_a)
    def copy_b(src, peer, step):
        pltpu.make_async_remote_copy(
            src_ref=src,
            dst_ref=got_b.at[me],
            send_sem=send_sem,
            recv_sem=recv_b.at[step // BATCH],
            device_id={"ch": peer},
            device_id_type=MESH,
        ).start()

    def send_b(step, carry):
        peer = lax.rem(me + step, groups)

        @pl.when(lax.rem(peer // BOX[3], BOX[2]) >= EARLY)
        def _():
            copy_b(sent_b.at[peer], peer, step)

        return carry

    per_layer = groups // BOX[2]
    place_in_layer = me // (BOX[2] * BOX[3]) * BOX[3] + core

    def early(k):
        there = lax.rem(place_in_layer + k % per_layer, per_layer)
        layer = k // per_layer
        return (there // BOX[3] * BOX[2] + layer) * BOX[3] + lax.rem(there, BOX[3])

    def pack_early(batch):
        for k in range(batch * BATCH, (batch + 1) * BATCH):
            rows = stage_b[pl.ds(early(k), samples, stride=PITCH_B), :]
            early_b[k] = rows.astype(jnp.bfloat16)

    def send_early(batch):
        for k in range(batch * BATCH, (batch + 1) * BATCH):
            peer = early(k)

            @pl.when(peer != me)
            def _(k=k, peer=peer):
                copy_b(early_b.at[k], peer, lax.rem(peer + groups - me, groups))

    def regrid_batch(batch):
        for j in range(BATCH):
            d = lax.rem(me + batch * BATCH + j, groups)
            blocks = [tiles[2 * d], tiles[2 * d + 1]]
            x = [fields[rows, block] for block in blocks for rows in range(fields.shape[0])]
            both = lax.dot_general(
                jnp.concatenate(x, axis=0), regrid[d], NT, preferred_element_type=jnp.float32
            )
            mine = jnp.where(left_half, both[:samples], both[samples:])
            sent_a[d] = mine.astype(jnp.bfloat16)

    load_tiles.wait()
    load_fields.wait()
    load_regrid[0].wait()
    ahead = batches // 4
    per_chunk = CHUNK // BATCH
    for batch in range(ahead):
        if batch % per_chunk == 0:
            load_regrid[batch // per_chunk + 1].wait()
        regrid_batch(batch)
    got_a[me] = sent_a[me]
    pl.semaphore_wait(barrier, groups - 1)
    sent = 0
    for batch in range(ahead, batches):
        if batch % per_chunk == 0 and batch // per_chunk + 1 < chunks:
            load_regrid[batch // per_chunk + 1].wait()
        regrid_batch(batch)
        ready = min(batch, sent + 2)
        lax.fori_loop(max(1, sent * BATCH), ready * BATCH, send_a, 0, unroll=True)
        sent = ready
    lax.fori_loop(sent * BATCH, groups, send_a, 0, unroll=True)

    for copy in load_dec:
        copy.wait()

    def decode(block, carry):
        first = block * TOGETHER
        v = latent[pl.ds(first, TOGETHER)].astype(jnp.float32).reshape(TOGETHER * nodes, -1)
        centred = v - jnp.mean(v, axis=1, keepdims=True)
        spread = jnp.mean(centred * centred, axis=1, keepdims=True)
        normed = (centred * lax.rsqrt(spread + EPSILON) * norm_b[...]).astype(jnp.bfloat16)
        middle = silu(jnp.dot(normed, dec_mid[...], preferred_element_type=jnp.float32))
        out = jnp.dot(
            middle.astype(jnp.bfloat16), dec_out[...], preferred_element_type=jnp.float32
        )
        for k in range(TOGETHER):
            rows = pl.ds(pl.multiple_of((first + k) * PITCH_B, 8), groups)
            stage_b[rows, :] = out[k * nodes : (k + 1) * nodes].T
        return carry

    lax.fori_loop(0, samples // TOGETHER, decode, 0)

    def pack_batch(batch, carry):
        for j in range(BATCH):
            c = lax.rem(me + batch * BATCH + j, groups)
            rows = stage_b[pl.ds(c, samples, stride=PITCH_B), :]
            sent_b[c] = rows.astype(jnp.bfloat16)
        return carry

    def pack_and_send(batch, carry):
        pack_batch(batch, carry)
        for j in range(BATCH):
            send_b((batch - 1) * BATCH + j, carry)
        return carry

    early_batches = EARLY * per_layer // BATCH
    pack_batch(0, 0)
    pack_batch(1, 0)
    lax.fori_loop(1, BATCH, send_b, 0, unroll=True)
    lax.fori_loop(2, 4, pack_and_send, 0)
    for batch in range(early_batches):
        pack_early(batch)
    for batch in range(early_batches):
        send_early(batch)
    lax.fori_loop(4, batches, pack_and_send, 0)
    lax.fori_loop(groups - BATCH, groups, send_b, 0, unroll=True)
    got_b[me] = sent_b[me]

    for copy in load_enc:
        copy.wait()
    most = pl.ds(0, groups - 1)
    pltpu.make_async_copy(sent_a.at[most], got_a.at[most], recv_a).wait()

    def add(c, total):
        return total + got_a[c].astype(jnp.float32)

    zero = jnp.zeros((samples, nodes), jnp.float32)
    average = lax.fori_loop(0, groups, add, zero, unroll=8) / groups

    def add_square(c, total):
        centred = got_a[c].astype(jnp.float32) - average
        return total + centred * centred

    spread = lax.fori_loop(0, groups, add_square, zero, unroll=8) / groups
    factor = lax.rsqrt(spread + EPSILON)

    def scale(c, carry):
        centred = got_a[c].astype(jnp.float32) - average
        rows = pl.ds(pl.multiple_of(c * PITCH_A, 8), samples)
        stage_a[rows, :] = centred * factor * norm_a[c]
        return carry

    lax.fori_loop(0, groups, scale, 0, unroll=8)

    def encode(block, carry):
        first = block * TOGETHER
        normed = jnp.concatenate(
            [stage_a[pl.ds(first + k, groups, stride=PITCH_A), :].T for k in range(TOGETHER)],
            axis=0,
        ).astype(jnp.bfloat16)
        base = jnp.dot(normed, enc_in[...], preferred_element_type=jnp.float32).astype(jnp.bfloat16)
        middle = silu(jnp.dot(base, enc_mid[...], preferred_element_type=jnp.float32))
        out = base.astype(jnp.float32) + jnp.dot(
            middle.astype(jnp.bfloat16), enc_out[...], preferred_element_type=jnp.float32
        )
        latent_o[pl.ds(first, TOGETHER)] = out.astype(jnp.bfloat16).reshape(TOGETHER, nodes, -1)
        return carry

    lax.fori_loop(0, samples // TOGETHER, encode, 0)

    def regrid_back(batch, carry):
        for j in range(BATCH):
            s = lax.rem(me + groups - batch * BATCH - j, groups)
            x = got_b[s]
            none = jnp.zeros_like(x)
            split = jnp.concatenate([jnp.where(left_half, x, none), jnp.where(left_half, none, x)], axis=0)
            cells = jnp.dot(split, regrid[s], preferred_element_type=jnp.float32)
            cells_o[s] = cells.astype(jnp.bfloat16)
        return carry

    def wait_back(batch, count):
        part = pl.ds(0, count)
        pltpu.make_async_copy(sent_b.at[part], got_b.at[part], recv_b.at[batch]).wait()

    wait_back(0, BATCH - 1)
    regrid_back(0, 0)

    def back(batch, carry):
        wait_back(batch, BATCH)
        return regrid_back(batch, carry)

    lax.fori_loop(1, batches, back, 0)
    for sent, got in ((sent_a, got_a), (sent_b, got_b)):
        pltpu.make_async_copy(sent.at[most], got.at[most], send_sem).wait()


def finish_body(tiles, latent, cells, latent_o, cells_o, placed, sem):
    copies = [pltpu.make_async_copy(latent, latent_o, sem.at[0])]
    copies[0].start()
    parts, rows = placed.shape[0], placed.shape[2]

    def place(s, carry):
        for half in range(2):
            to = tiles[2 * s + half]
            for part in range(parts):
                first = (half * parts + part) * rows
                placed[part, to] = cells[s, first : first + rows]
        return carry

    lax.fori_loop(0, cells.shape[0], place, 0, unroll=8)
    copies.append(pltpu.make_async_copy(placed, cells_o, sem.at[1]))
    copies[1].start()
    for copy in copies:
        copy.wait()


def shards(
    fields_a,
    latent_b,
    regrid_w,
    cell_tiles,
    norm_a,
    enc_in,
    enc_mid,
    enc_out,
    norm_b,
    dec_mid,
    dec_out,
):
    groups = lax.axis_size("ch")
    samples, nodes, hidden = latent_b.shape
    all_cells = fields_a.shape[2]
    bf16, f32 = jnp.bfloat16, jnp.float32
    tiles = cell_tiles.reshape(-1)
    fields = jnp.swapaxes(fields_a.reshape(samples // 8, 8, all_cells // BC, BC), 1, 2)
    regrid = jnp.swapaxes(regrid_w, 2, 3).reshape(groups, 2 * BN, BC)
    args = (
        tiles,
        fields,
        regrid,
        latent_b,
        norm_a,
        enc_in,
        enc_mid,
        enc_out,
        norm_b.reshape(1, -1),
        dec_mid,
        dec_out,
    )
    hbm = pl.BlockSpec(memory_space=pltpu.HBM)
    vmem = pl.BlockSpec(memory_space=pltpu.VMEM)
    smem = pl.BlockSpec(memory_space=pltpu.SMEM)
    message = pltpu.VMEM((groups, samples, nodes), bf16)
    latent_a, cells, tiles = pl.pallas_call(
        functools.partial(main_body, groups),
        out_shape=[
            pltpu.VMEM((samples, nodes, hidden), bf16),
            pltpu.VMEM((groups, 2 * samples, BC), bf16),
            pltpu.SMEM(tiles.shape, jnp.int32),
        ],
        in_specs=[hbm] * 11,
        out_specs=[vmem, vmem, smem],
        scratch_shapes=[
            pltpu.SMEM(norm_a.shape, f32),
            pltpu.VMEM(fields.shape, bf16),
            pltpu.VMEM(regrid.shape, bf16),
            pltpu.VMEM(latent_b.shape, bf16),
            pltpu.VMEM(enc_in.shape, bf16),
            pltpu.VMEM(enc_mid.shape, bf16),
            pltpu.VMEM(enc_out.shape, bf16),
            pltpu.VMEM((1, hidden), f32),
            pltpu.VMEM(dec_mid.shape, bf16),
            pltpu.VMEM(dec_out.shape, bf16),
            message,
            message,
            pltpu.VMEM((EARLY * groups // BOX[2], samples, nodes), bf16),
            message,
            message,
            pltpu.VMEM((groups * PITCH_A, nodes), f32),
            pltpu.VMEM((samples * PITCH_B, nodes), f32),
            pltpu.SemaphoreType.DMA((10,)),
            pltpu.SemaphoreType.DMA((groups // CHUNK,)),
            pltpu.SemaphoreType.DMA,
            pltpu.SemaphoreType.DMA,
            pltpu.SemaphoreType.DMA((groups // BATCH,)),
        ],
        compiler_params=pltpu.CompilerParams(
            collective_id=0, has_side_effects=True, vmem_limit_bytes=40 * 2**20
        ),
        name="main",
    )(*map(in_hbm, args))
    latent_a, cells_b = pl.pallas_call(
        finish_body,
        out_shape=[
            pltpu.HBM(latent_a.shape, bf16),
            pltpu.HBM(fields.shape, bf16),
        ],
        in_specs=[smem, vmem, vmem],
        out_specs=[hbm, hbm],
        scratch_shapes=[
            pltpu.VMEM(fields.shape, bf16),
            pltpu.SemaphoreType.DMA((2,)),
        ],
        name="finish",
    )(in_smem(tiles), in_vmem(latent_a), in_vmem(cells))
    return latent_a, jnp.swapaxes(cells_b, 1, 2).reshape(samples, 1, all_cells)


def solution(mesh):
    sharded = P("rep", "ch", None)
    return jax.shard_map(
        shards,
        mesh=mesh,
        in_specs=(sharded, sharded) + (P(),) * 9,
        out_specs=(sharded, sharded),
        check_vma=False,
    )
```
